16 devices in a mesh: dp: 4 (over y, z, core), tp: 4 (over x).
Axes of the slice: x: 4, y: 2, z: 1, core: 2. Of those that a mesh axis runs over, the one named last changes fastest.
The devices are a block of a 4x4x8 slice.
Arguments:
- x: bfloat16 [4096, 4096], P(('dp', 'tp')), parts along dimension 0
- dy: bfloat16 [4096, 4096], P(('dp', 'tp')), parts along dimension 0
- pre: bfloat16 [4096, 16384], P('dp', 'tp'), parts along dimension 0
- w_in: bfloat16 [4096, 16384], P(None, 'tp')
- w_down: bfloat16 [16384, 4096], P('tp')
Outputs:
- output 1: bfloat16 [4096, 4096], P(('dp', 'tp')), parts along dimension 0
- output 2: bfloat16 [16384, 16384], P('dp', 'tp'), parts along dimension 0
- output 3: bfloat16 [65536, 4096], P(('dp', 'tp')), parts along dimension 0
There are 4 independent parts. The reference program is written for one: setup_inputs(seed, part) draws one part's arguments, and reference() takes and returns one part's arrays. A program takes and returns all parts, laid end to end along the dimension named above; an argument that names none is the same for every part.
All inputs are finite; a program needn't handle non-finite values.
Results may differ from the reference program's by a relative error of at most 0.012.
Values are sent between devices in bfloat16 or wider.
A program may use at most 768 MiB of HBM per device.

```python
import jax
import jax.numpy as jnp

ROWS = 1024
D = 4096
FF = 16384


def act(pre):
    return jax.nn.gelu(pre)


def setup_inputs(seed: int = 0, part: int = 0) -> dict:
    kx, ky, ka, ki, kd = jax.random.split(jax.random.key(seed), 5)
    kx, ky, ka = (jax.random.fold_in(k, part) for k in (kx, ky, ka))
    drawn = {
        "x": jax.random.normal(kx, (ROWS, D), jnp.float32),
        "dy": jax.random.normal(ky, (ROWS, D), jnp.float32),
        "pre": jax.random.normal(ka, (ROWS, FF), jnp.float32),
        "w_in": jax.random.normal(ki, (D, FF), jnp.float32) * D**-0.5,
        "w_down": jax.random.normal(kd, (FF, D), jnp.float32) * FF**-0.5,
    }
    return {k: v.astype(jnp.bfloat16) for k, v in drawn.items()}


def reference(x, dy, pre, w_in, w_down):
    hidden, back = jax.vjp(act, pre.astype(jnp.float32))
    d_hidden = jnp.dot(dy, w_down.T, preferred_element_type=jnp.float32)
    d_pre = back(d_hidden)[0].astype(jnp.bfloat16)
    dx = jnp.dot(d_pre, w_in.T, preferred_element_type=jnp.float32)
    dw_in = jnp.dot(x.T, d_pre, preferred_element_type=jnp.float32)
    dw_down = jnp.dot(hidden.astype(jnp.bfloat16).T, dy, preferred_element_type=jnp.float32)
    return tuple(g.astype(jnp.bfloat16) for g in (dx, dw_in, dw_down))
```

```python
import functools

import jax
import jax.numpy as jnp
from jax import lax
from jax.experimental import pallas as pl
from jax.experimental.pallas import tpu as pltpu
from jax.sharding import PartitionSpec as P


F32, BF16 = jnp.float32, jnp.bfloat16

C0 = 0.7978845608028654
C1 = 0.044715


def nt(a, b):
    return lax.dot_general(a, b, (((1,), (1,)), ((), ())), preferred_element_type=F32)


def cost(flops, nbytes):
    return pl.CostEstimate(flops=int(flops), bytes_accessed=int(nbytes), transcendentals=0)


def gelu_and_slope(x):
    xx = x * x
    t = jnp.tanh(x * (C0 + (C0 * C1) * xx))
    cdf = 0.5 + 0.5 * t
    return x * cdf, cdf + (0.5 * ((1.0 - t * t) * x)) * (C0 + (3.0 * C0 * C1) * xx)


def stage_kernel(n_dy, n_out, order, *refs):
    dys, (pre, w_down, w_in), rest = refs[:n_dy], refs[n_dy : n_dy + 3], refs[n_dy + 3 :]
    (hid, d_pre), outs, scratch = rest[:2], rest[2 : 2 + n_out], rest[2 + n_out :]
    lhs, w_buf, pre_buf, d_buf, hid_buf, out_buf, lhs_sem, w_sem, pre_sem, d_sem, hid_sem, out_sem = scratch
    rows = lhs.shape[0]
    half = rows // 2
    _, chunks, chunk, _ = w_buf.shape
    block = chunks * chunk
    steps = w_down.shape[0] // block
    steps_x = w_in.shape[0] // block

    def weights(b):
        slot = lax.rem(b, 2)

        def each(src, at):
            for c in range(chunks):
                copy = pltpu.make_async_copy(
                    src.at[pl.ds(at + c * chunk, chunk), :], w_buf.at[slot, c], w_sem.at[slot, c]
                )
                copy.start()

        @pl.when(b < steps)
        def _():
            each(w_down, b * block)

        @pl.when((b >= steps) & (b < steps + steps_x))
        def _():
            each(w_in, (b - steps) * block)

    def weights_wait(slot, c):
        pltpu.make_async_copy(w_down.at[pl.ds(0, chunk), :], w_buf.at[slot, c], w_sem.at[slot, c]).wait()

    def pre_copies(j):
        slot = lax.rem(j, 2)
        return [
            pltpu.make_async_copy(
                pre.at[pl.ds(pl.multiple_of(order[k] * half, half), half), pl.ds(pl.multiple_of(j * block, block), block)],
                pre_buf.at[slot, pl.ds(k * half, half), :],
                pre_sem.at[slot, k],
            )
            for k in range(2)
        ]

    def hid_copy(j):
        slot = lax.rem(j, 2)
        return pltpu.make_async_copy(hid_buf.at[slot], hid.at[pl.ds(j * block, block), :], hid_sem.at[slot])

    def out_copies(j):
        slot = lax.rem(j, 2)
        at, copies = 0, []
        for k, o in enumerate(outs):
            n = o.shape[0]
            copies.append(
                pltpu.make_async_copy(
                    out_buf.at[slot, pl.ds(at, n), :],
                    o.at[:, pl.ds(pl.multiple_of(j * block, block), block)],
                    out_sem.at[slot, k],
                )
            )
            at += n
        return copies

    lhs_copies, at = [], 0
    for k, d in enumerate(dys):
        lhs_copies.append(pltpu.make_async_copy(d, lhs.at[pl.ds(at, d.shape[0]), :], lhs_sem.at[k]))
        at += d.shape[0]
    for copy in lhs_copies:
        copy.start()
    weights(0)
    for copy in pre_copies(0):
        copy.start()
    for copy in lhs_copies:
        copy.wait()

    def first(j, _):
        slot = lax.rem(j, 2)
        weights(j + 1)

        @pl.when(j + 1 < steps)
        def _():
            for copy in pre_copies(j + 1):
                copy.start()

        for copy in pre_copies(j):
            copy.wait()

        @pl.when(j >= 2)
        def _():
            hid_copy(j - 2).wait()

        for c in range(chunks):
            weights_wait(slot, c)
        for c in range(chunks):
            d_hid = nt(lhs[...], w_buf[slot, c])
            h, slope = gelu_and_slope(pre_buf[slot, :, c * chunk : (c + 1) * chunk].astype(F32))
            hid_buf[slot, c * chunk : (c + 1) * chunk, :] = h.T.astype(BF16)
            d_buf[:, pl.ds(pl.multiple_of(j * block + c * chunk, chunk), chunk)] = (d_hid * slope).astype(BF16)
        hid_copy(j).start()
        return 0

    lax.fori_loop(0, steps, first, 0)
    d_copy = pltpu.make_async_copy(d_buf, d_pre, d_sem)
    d_copy.start()

    def second(j, _):
        slot = lax.rem(j + steps, 2)
        weights(j + steps + 1)

        @pl.when(j >= 2)
        def _():
            for copy in out_copies(j - 2):
                copy.wait()

        for c in range(chunks):
            weights_wait(slot, c)
        for c in range(chunks):
            out_buf[lax.rem(j, 2), :, c * chunk : (c + 1) * chunk] = nt(d_buf[...], w_buf[slot, c]).astype(out_buf.dtype)
        for copy in out_copies(j):
            copy.start()
        return 0

    lax.fori_loop(0, steps_x, second, 0)
    d_copy.wait()
    for j in range(max(steps - 2, 0), steps):
        hid_copy(j).wait()
    for j in range(max(steps_x - 2, 0), steps_x):
        for copy in out_copies(j):
            copy.wait()


def stage_of(order, dys, pre, w_down, w_in, outs, dtype):
    rows = sum(d.shape[0] for d in dys)
    ff, d = w_down.shape
    chunk, chunks = 512, 2
    block = chunk * chunks
    anywhere = pl.BlockSpec(memory_space=pl.ANY)
    out_shape = [jax.ShapeDtypeStruct((ff, rows), BF16), jax.ShapeDtypeStruct((rows, ff), BF16)]
    out_shape += [jax.ShapeDtypeStruct((r, d), dtype) for r in outs]
    dma = pltpu.SemaphoreType.DMA
    return pl.pallas_call(
        functools.partial(stage_kernel, len(dys), len(outs)),
        grid_spec=pltpu.PrefetchScalarGridSpec(
            num_scalar_prefetch=1,
            grid=(),
            in_specs=[anywhere] * (len(dys) + 3),
            out_specs=[anywhere] * len(out_shape),
            scratch_shapes=[
                pltpu.VMEM((rows, d), BF16),
                pltpu.VMEM((2, chunks, chunk, d), BF16),
                pltpu.VMEM((2, rows, block), BF16),
                pltpu.VMEM((rows, ff), BF16),
                pltpu.VMEM((2, block, rows), BF16),
                pltpu.VMEM((2, rows, block), dtype),
                dma((len(dys),)),
                dma((2, chunks)),
                dma((2, 2)),
                dma,
                dma((2,)),
                dma((2, len(outs))),
            ],
        ),
        out_shape=out_shape,
        cost_estimate=cost(4 * rows * ff * d, 4 * ff * d),
    )(order, *dys, pre, w_down, w_in)


def dw_kernel(n_lhs, n_rhs, turn, *refs):
    lhs_refs, rhs_refs = refs[:n_lhs], refs[n_lhs : n_lhs + n_rhs]
    o_ref, lhs = refs[-2:]

    @pl.when(pl.program_id(1) == 0)
    def _():
        at = 0
        for r in lhs_refs:
            n = r.shape[0] if turn else r.shape[1]
            lhs[:, at : at + n] = r[...].T if turn else r[...]
            at += n

    rhs = jnp.concatenate([r[...] for r in rhs_refs], axis=0)
    o_ref[...] = jnp.dot(lhs[...], rhs, preferred_element_type=F32).astype(BF16)


def dw_of(lhs, rhs, turn, part=0, parts=1, into=None):
    m, n = lhs[0].shape[1 if turn else 0], rhs[0].shape[1]
    k = sum(t.shape[0] for t in rhs)
    bm, bn = min(1024, m // parts), min(2048, n)
    steps = m // parts // bm
    first = part * steps
    more = [] if into is None else [into]
    if turn:
        lhs_specs = [pl.BlockSpec((t.shape[0], bm), lambda i, j: (0, first + i)) for t in lhs]
    else:
        lhs_specs = [pl.BlockSpec((bm, t.shape[1]), lambda i, j: (first + i, 0)) for t in lhs]
    return pl.pallas_call(
        functools.partial(dw_kernel, len(lhs), len(rhs), turn),
        grid=(steps, n // bn),
        in_specs=lhs_specs
        + [pl.BlockSpec((t.shape[0], bn), lambda i, j: (0, j)) for t in rhs]
        + [pl.BlockSpec(memory_space=pl.ANY) for _ in more],
        out_specs=pl.BlockSpec((bm, bn), lambda i, j: (first + i, j)),
        out_shape=jax.ShapeDtypeStruct((m, n), BF16),
        scratch_shapes=[pltpu.VMEM((bm, k), BF16)],
        input_output_aliases={len(lhs) + len(rhs): 0} if more else {},
        cost_estimate=cost(2 * m * n * k // parts, 2 * m * n // parts),
    )(*lhs, *rhs, *more)


def last_kernel(own_ref, from_right, over_left, from_left, over_right, o_ref):
    half = from_right.shape[0]
    o_ref[:half, :] = (
        own_ref[:half, :] + from_right[...].astype(F32) + over_left[...].astype(F32)
    ).astype(BF16)
    o_ref[half:, :] = (
        own_ref[half:, :] + from_left[...].astype(F32) + over_right[...].astype(F32)
    ).astype(BF16)


def last_sum(own, from_right, over_left, from_left, over_right):
    rows, d = own.shape
    half, bd = rows // 2, min(1024, d)
    piece = pl.BlockSpec((half, bd), lambda j: (0, j))
    whole = pl.BlockSpec((rows, bd), lambda j: (0, j))
    return pl.pallas_call(
        last_kernel,
        grid=(d // bd,),
        in_specs=[whole, piece, piece, piece, piece],
        out_specs=whole,
        out_shape=jax.ShapeDtypeStruct((rows, d), BF16),
        cost_estimate=cost(rows * d * 100, rows * d * 10),
    )(own, from_right, over_left, from_left, over_right)


def solution(mesh):
    n = mesh.shape["tp"]
    to_right = [(i, (i + 1) % n) for i in range(n)]
    to_left = [(i, (i - 1) % n) for i in range(n)]

    def right(t):
        return lax.ppermute(t, "tp", to_right)

    def left(t):
        return lax.ppermute(t, "tp", to_left)

    def step(x, dy, pre, w_in, w_down):
        half = dy.shape[0] // 2
        me = lax.axis_index("tp")
        l, r, o = (me + n - 1) % n, (me + 1) % n, (me + 2) % n
        orders = [(2 * me, 2 * me + 1), (2 * l, 2 * r + 1), (2 * l + 1, 2 * r), (2 * o, 2 * o + 1)]
        orders = [jnp.stack(t) for t in orders]

        dy_a, dy_b = dy[:half], dy[half:]
        dy_la = right(dy_a)
        dy_rb = left(dy_b)
        dy_lb = right(dy_b)
        dy_ra = left(dy_a)
        dy_oa = right(dy_la)
        dy_ob = left(dy_rb)

        x_a, x_b = x[:half], x[half:]
        x_la = right(x_a)
        x_rb = left(x_b)
        x_lb = right(x_b)
        x_ra = left(x_a)
        x_oa = right(x_la)
        x_ob = left(x_rb)

        weights = pre, w_down, w_in
        h0, d0, own = stage_of(orders[0], [dy], *weights, [2 * half], F32)
        h1, d1, p_la, p_rb = stage_of(orders[1], [dy_la, dy_rb], *weights, [half, half], BF16)
        h2, d2, p_lb, p_ra = stage_of(orders[2], [dy_lb, dy_ra], *weights, [half, half], F32)
        h3, d3, p_oa, p_ob = stage_of(orders[3], [dy_oa, dy_ob], *weights, [half, half], BF16)

        in_l = right(p_oa)
        in_r = left(p_ob)
        from_left = right(p_rb)
        from_right = left(p_la)
        over_left = right((p_ra + in_l.astype(F32)).astype(BF16))
        over_right = left((p_lb + in_r.astype(F32)).astype(BF16))

        dys = [dy, dy_la, dy_rb, dy_lb, dy_ra, dy_oa, dy_ob]
        dw_down = dw_of([h0, h1, h2, h3], dys, False)
        xs, d_pre = [x, x_la, x_rb, x_lb, x_ra, x_oa, x_ob], [d0, d1, d2, d3]
        dw_in = dw_of(xs, d_pre, True, 0, 2)
        dw_in = dw_of(xs, d_pre, True, 1, 2, dw_in)
        dx = last_sum(own, from_right, over_left, from_left, over_right)
        return dx, dw_in, dw_down

    return jax.shard_map(
        step,
        mesh=mesh,
        in_specs=(P(("dp", "tp"), None), P(("dp", "tp"), None), P("dp", "tp"), P(None, "tp"), P("tp", None)),
        out_specs=(P(("dp", "tp"), None), P("dp", "tp"), P(("dp", "tp"), None)),
        check_vma=False,
    )
```

```python
import functools

import jax
import jax.numpy as jnp
from jax import lax
from jax.experimental import pallas as pl
from jax.experimental.pallas import tpu as pltpu
from jax.sharding import PartitionSpec as P


F32, BF16 = jnp.float32, jnp.bfloat16

C0 = 0.7978845608028654
C1 = 0.044715


def nt(a, b):
    return lax.dot_general(a, b, (((1,), (1,)), ((), ())), preferred_element_type=F32)


def cost(flops, nbytes):
    return pl.CostEstimate(flops=int(flops), bytes_accessed=int(nbytes), transcendentals=0)


def gelu_and_slope(x):
    xx = x * x
    t = jnp.tanh(x * (C0 + (C0 * C1) * xx))
    cdf = 0.5 + 0.5 * t
    return x * cdf, cdf + (0.5 * ((1.0 - t * t) * x)) * (C0 + (3.0 * C0 * C1) * xx)


def front_kernel(n, x, dy, pre, w_in, w_down, hid, d_pre, dy_all, x_la, x_rb, x_a, x_b, own, p_la, p_rb, p_lb, p_ra, p_oa, p_ob, *scratch):
    dy_buf, w_all, w_buf, pre_buf, x_buf, d_buf, hid_buf, out_wide, out_slim = scratch[:9]
    send_sem, recv_sem, own_sem, all_sem, w_sem, pre_sem, d_sem, hid_sem, out_sem, dy_sem, x_sem, turn_sem = scratch[9:]
    me = lax.axis_index("tp")
    right, left, far = lax.rem(me + 1, n), lax.rem(me + n - 1, n), lax.rem(me + 2, n)
    pieces, piece, _ = w_all.shape
    slots = w_buf.shape[0]
    block = 2 * piece
    steps = pieces // 2
    rows = dy.shape[0]
    half = rows // 2
    total = 4 * pieces

    barrier = pltpu.get_barrier_semaphore()
    for neighbour in (left, right):
        pl.semaphore_signal(barrier, inc=1, device_id={"tp": neighbour}, device_id_type=pl.DeviceIdType.MESH)
    pl.semaphore_wait(barrier, 2)

    def send(k, src, dst, to):
        return pltpu.make_async_remote_copy(
            src_ref=src,
            dst_ref=dst,
            send_sem=send_sem.at[k],
            recv_sem=recv_sem.at[k],
            device_id={"tp": to},
            device_id_type=pl.DeviceIdType.MESH,
        )

    up, down = pl.ds(0, half), pl.ds(half, half)
    sends = [
        send(0, dy.at[up], dy_buf.at[1, up], right),
        send(1, dy.at[down], dy_buf.at[1, down], left),
        send(2, dy.at[down], dy_buf.at[2, up], right),
        send(3, dy.at[up], dy_buf.at[2, down], left),
        send(4, dy_buf.at[1, up], dy_buf.at[3, up], right),
        send(5, dy_buf.at[1, down], dy_buf.at[3, down], left),
        send(6, x_a, x_la, right),
        send(7, x_b, x_rb, left),
    ]
    for k in range(4):
        sends[k].start()

    def columns(j):
        return pl.ds(pl.multiple_of(j * block, block), block)

    def whole_copy(j):
        return pltpu.make_async_copy(w_down.at[pl.ds(pl.multiple_of(j * piece, piece), piece)], w_all.at[j], all_sem.at[j])

    def w_copy(b):
        at = pl.multiple_of(lax.rem(b, pieces) * piece, piece)
        slot = lax.rem(b, slots)
        return pltpu.make_async_copy(w_in.at[pl.ds(at, piece)], w_buf.at[slot], w_sem.at[slot])

    first_rows = [
        (2 * me, 2 * me + 1),
        (2 * left, 2 * right + 1),
        (2 * left + 1, 2 * right),
        (2 * far, 2 * far + 1),
    ]

    def pre_copies(s, j):
        slot = lax.rem(j, 2)
        return [
            pltpu.make_async_copy(
                pre.at[pl.ds(pl.multiple_of(first_rows[s][k] * half, half), half), columns(j)],
                pre_buf.at[slot, pl.ds(k * half, half)],
                pre_sem.at[slot, k],
            )
            for k in range(2)
        ]

    def hid_copy(s, j):
        return pltpu.make_async_copy(hid_buf, hid.at[columns(j), pl.ds(s * rows, rows)], hid_sem)

    def x_copy(j):
        return pltpu.make_async_copy(x.at[:, columns(j)], x_buf, x_sem)

    def turn_copies(j):
        return [
            pltpu.make_async_copy(hid_buf.at[:, up], x_a.at[columns(j)], turn_sem.at[0]),
            pltpu.make_async_copy(hid_buf.at[:, down], x_b.at[columns(j)], turn_sem.at[1]),
        ]

    outs_of = [(own,), (p_la, p_rb), (p_lb, p_ra), (p_oa, p_ob)]

    def out_copies(s, j):
        buf = out_wide if s % 2 == 0 else out_slim
        at, copies = 0, []
        for k, o in enumerate(outs_of[s]):
            copies.append(pltpu.make_async_copy(buf.at[pl.ds(at, o.shape[0])], o.at[:, columns(j)], out_sem.at[k]))
            at += o.shape[0]
        return copies

    own_copy = pltpu.make_async_copy(dy, dy_buf.at[0], own_sem)
    own_copy.start()
    for copy in pre_copies(0, 0):
        copy.start()
    for j in range(pieces):
        whole_copy(j).start()
    x_copy(0).start()
    own_copy.wait()

    for s in range(4):
        if s > 0:
            for k in (2 * s - 2, 2 * s - 1):
                sends[k].wait_recv()
            if s == 1:
                for k in range(4, 8):
                    sends[k].start()
            keep = pltpu.make_async_copy(dy_buf.at[s], dy_all.at[pl.ds((s - 1) * rows, rows)], dy_sem.at[s - 1])
            keep.start()

        def first(j, _, s=s):
            slot = lax.rem(j, 2)

            @pl.when(j + 1 < steps)
            def _():
                for copy in pre_copies(s, j + 1):
                    copy.start()

            if s == 0:
                for c in range(2):
                    whole_copy(2 * j + c).wait()

                @pl.when(2 * j + slots >= pieces)
                def _():
                    for c in range(2):
                        w_copy(2 * j + c + slots - pieces).start()

            for copy in pre_copies(s, j):
                copy.wait()

            @pl.when(j >= 1)
            def _():
                hid_copy(s, j - 1).wait()

            for c in range(2):
                d_hid = nt(dy_buf[s], w_all[2 * j + c])
                h, slope = gelu_and_slope(pre_buf[slot, :, c * piece : (c + 1) * piece].astype(F32))
                hid_buf[c * piece : (c + 1) * piece, :] = h.T.astype(BF16)
                d_buf[:, pl.ds(pl.multiple_of(j * block + c * piece, piece), piece)] = (d_hid * slope).astype(BF16)
            hid_copy(s, j).start()
            return 0

        lax.fori_loop(0, steps, first, 0)
        d_copy = pltpu.make_async_copy(d_buf, d_pre.at[pl.ds(s * rows, rows)], d_sem)
        d_copy.start()
        if s < 3:
            for copy in pre_copies(s + 1, 0):
                copy.start()
        hid_copy(s, steps - 1).wait()

        def second(j, _, s=s):
            b = s * pieces + 2 * j
            if s == 0:
                x_copy(j).wait()
            for c in range(2):
                w_copy(b + c).wait()

            @pl.when(j >= 1)
            def _():
                for copy in out_copies(s, j - 1):
                    copy.wait()
                if s == 0:
                    for copy in turn_copies(j - 1):
                        copy.wait()

            buf = out_wide if s % 2 == 0 else out_slim
            for c in range(2):
                part = nt(d_buf[...], w_buf[lax.rem(b + c, slots)])
                buf[:, c * piece : (c + 1) * piece] = part.astype(buf.dtype)
            if s == 0:
                hid_buf[...] = x_buf[...].T
                for copy in turn_copies(j):
                    copy.start()

                @pl.when(j + 1 < steps)
                def _():
                    x_copy(j + 1).start()

            for copy in out_copies(s, j):
                copy.start()

            @pl.when(b + slots < total)
            def _():
                for c in range(2):
                    w_copy(b + c + slots).start()

            return 0

        lax.fori_loop(0, steps, second, 0)
        for copy in out_copies(s, steps - 1):
            copy.wait()
        if s == 0:
            for copy in turn_copies(steps - 1):
                copy.wait()
        d_copy.wait()
        if s > 0:
            keep.wait()

    for k in (6, 7):
        sends[k].wait_recv()
    for k in range(8):
        sends[k].wait_send()


def front(n, x, dy, pre, w_in, w_down):
    rows, d = dy.shape
    tokens, ff = pre.shape
    half, piece, slots = rows // 2, 512, 4
    pieces, block = ff // piece, 2 * piece
    anywhere = pl.BlockSpec(memory_space=pl.ANY)
    dma = pltpu.SemaphoreType.DMA
    shapes = [((ff, tokens), BF16), ((tokens, ff), BF16), ((tokens - rows, d), BF16)]
    shapes += [((d, half), BF16)] * 4 + [((rows, d), F32)]
    shapes += [((half, d), BF16)] * 2 + [((half, d), F32)] * 2 + [((half, d), BF16)] * 2
    out_shape = [jax.ShapeDtypeStruct(*t) for t in shapes]
    return pl.pallas_call(
        functools.partial(front_kernel, n),
        in_specs=[anywhere] * 5,
        out_specs=[anywhere] * len(out_shape),
        scratch_shapes=[
            pltpu.VMEM((4, rows, d), BF16),
            pltpu.VMEM((pieces, piece, d), BF16),
            pltpu.VMEM((slots, piece, ff), BF16),
            pltpu.VMEM((2, rows, block), BF16),
            pltpu.VMEM((rows, block), BF16),
            pltpu.VMEM((rows, ff), BF16),
            pltpu.VMEM((block, rows), BF16),
            pltpu.VMEM((rows, block), F32),
            pltpu.VMEM((rows, block), BF16),
            dma((8,)),
            dma((8,)),
            dma,
            dma((pieces,)),
            dma((slots,)),
            dma((2, 2)),
            dma,
            dma,
            dma((2,)),
            dma((3,)),
            dma,
            dma((2,)),
        ],
        out_shape=out_shape,
        compiler_params=pltpu.CompilerParams(collective_id=0, has_side_effects=True, vmem_limit_bytes=67043328),
        cost_estimate=cost(4 * tokens * ff * d, 10 * ff * d),
        name="front",
    )(x, dy, pre, w_in, w_down)


def dw_kernel(n_lhs, n_rhs, *refs):
    lhs = [r[...] for r in refs[:n_lhs]]
    rhs = [r[...] for r in refs[n_lhs : n_lhs + n_rhs]]
    lhs = lhs[0] if n_lhs == 1 else jnp.concatenate(lhs, axis=1)
    rhs = rhs[0] if n_rhs == 1 else jnp.concatenate(rhs, axis=0)
    refs[-1][...] = jnp.dot(lhs, rhs, preferred_element_type=F32).astype(BF16)


def dw_of(lhs, rhs, room, part=0, parts=1, into=None):
    m, n = lhs[0].shape[0], rhs[0].shape[1]
    k = sum(t.shape[0] for t in rhs)
    bm, bn = min(1024, m // parts), min(2048, n)
    steps = m // parts // bm
    first = part * steps
    more = [] if into is None else [into]
    return pl.pallas_call(
        functools.partial(dw_kernel, len(lhs), len(rhs)),
        grid=(steps, n // bn),
        in_specs=[pl.BlockSpec((bm, t.shape[1]), lambda i, j: (first + i, 0)) for t in lhs]
        + [pl.BlockSpec((t.shape[0], bn), lambda i, j: (0, j)) for t in rhs]
        + [pl.BlockSpec(memory_space=pl.ANY) for _ in more],
        out_specs=pl.BlockSpec((bm, bn), lambda i, j: (first + i, j)),
        out_shape=jax.ShapeDtypeStruct((m, n), BF16),
        input_output_aliases={len(lhs) + len(rhs): 0} if more else {},
        compiler_params=pltpu.CompilerParams(vmem_limit_bytes=room << 20),
        cost_estimate=cost(2 * m * n * k // parts, 2 * m * n // parts),
    )(*lhs, *rhs, *more)


def last_kernel(sum_ref, over_left, over_right, o_ref):
    half = over_left.shape[0]
    o_ref[:half, :] = (sum_ref[:half, :] + over_left[...].astype(F32)).astype(BF16)
    o_ref[half:, :] = (sum_ref[half:, :] + over_right[...].astype(F32)).astype(BF16)


def near_kernel(own_ref, from_right, from_left, o_ref):
    half = from_left.shape[0]
    o_ref[:half, :] = own_ref[:half, :] + from_right[...].astype(F32)
    o_ref[half:, :] = own_ref[half:, :] + from_left[...].astype(F32)


def sum_of(kernel, whole, top, low, dtype):
    rows, d = whole.shape
    half, bd = rows // 2, min(1024, d)
    piece = pl.BlockSpec((half, bd), lambda j: (0, j))
    full = pl.BlockSpec((rows, bd), lambda j: (0, j))
    return pl.pallas_call(
        kernel,
        grid=(d // bd,),
        in_specs=[full, piece, piece],
        out_specs=full,
        out_shape=jax.ShapeDtypeStruct((rows, d), dtype),
        compiler_params=pltpu.CompilerParams(vmem_limit_bytes=16 << 20),
        cost_estimate=cost(rows * d * 100, rows * d * 10),
    )(whole, top, low)


def solution(mesh):
    n = mesh.shape["tp"]
    to_right = [(i, (i + 1) % n) for i in range(n)]
    to_left = [(i, (i - 1) % n) for i in range(n)]

    def right(t):
        return lax.ppermute(t, "tp", to_right)

    def left(t):
        return lax.ppermute(t, "tp", to_left)

    def step(x, dy, pre, w_in, w_down):
        (hid, d_pre, dy_all, x_la, x_rb, x_a, x_b, own, p_la, p_rb, p_lb, p_ra, p_oa, p_ob) = front(
            n, x, dy, pre, w_in, w_down
        )
        x_lb = right(x_b)
        x_ra = left(x_a)
        x_oa = right(x_la)
        x_ob = left(x_rb)

        in_l = right(p_oa)
        in_r = left(p_ob)
        from_left = right(p_rb)
        from_right = left(p_la)
        over_left = right((p_ra + in_l.astype(F32)).astype(BF16))
        over_right = left((p_lb + in_r.astype(F32)).astype(BF16))

        dw_down = dw_of([hid], [dy, dy_all], 50)
        xs = [x_a, x_b, x_la, x_rb, x_lb, x_ra, x_oa, x_ob]
        dw_in = dw_of(xs, [d_pre], 28, 0, 2)
        dw_in = dw_of(xs, [d_pre], 28, 1, 2, dw_in)
        near = sum_of(near_kernel, own, from_right, from_left, F32)
        dx = sum_of(last_kernel, near, over_left, over_right, BF16)
        return dx, dw_in, dw_down

    return jax.shard_map(
        step,
        mesh=mesh,
        in_specs=(P(("dp", "tp"), None), P(("dp", "tp"), None), P("dp", "tp"), P(None, "tp"), P("tp", None)),
        out_specs=(P(("dp", "tp"), None), P("dp", "tp"), P(("dp", "tp"), None)),
        check_vma=False,
    )
```

```python
import functools

import jax
import jax.numpy as jnp
from jax import lax
from jax.experimental import pallas as pl
from jax.experimental.pallas import tpu as pltpu
from jax.sharding import PartitionSpec as P


F32, BF16 = jnp.float32, jnp.bfloat16

C0 = 0.7978845608028654
C1 = 0.044715


def nt(a, b):
    return lax.dot_general(a, b, (((1,), (1,)), ((), ())), preferred_element_type=F32)


def cost(flops, nbytes):
    return pl.CostEstimate(flops=int(flops), bytes_accessed=int(nbytes), transcendentals=0)


def gelu_and_slope(x):
    xx = x * x
    t = jnp.tanh(x * (C0 + (C0 * C1) * xx))
    cdf = 0.5 + 0.5 * t
    return x * cdf, cdf + (0.5 * ((1.0 - t * t) * x)) * (C0 + (3.0 * C0 * C1) * xx)


def front_kernel(n, x, dy, pre, w_in, w_down, hid, d_pre, dy_all, x_la, x_rb, x_a, x_b, own, p_la, p_rb, p_lb, p_ra, p_oa, p_ob, *scratch):
    dy_buf, w_all, w_buf, pre_buf, x_buf, d_buf, hid_buf, out_wide, out_slim = scratch[:9]
    send_sem, recv_sem, own_sem, all_sem, w_sem, pre_sem, d_sem, hid_sem, out_sem, dy_sem, x_sem, turn_sem = scratch[9:]
    me = lax.axis_index("tp")
    right, left, far = lax.rem(me + 1, n), lax.rem(me + n - 1, n), lax.rem(me + 2, n)
    pieces, piece, _ = w_all.shape
    slots = w_buf.shape[0]
    block = 2 * piece
    steps = pieces // 2
    rows = dy.shape[0]
    half = rows // 2
    total = 4 * pieces

    barrier = pltpu.get_barrier_semaphore()
    for neighbour in (left, right):
        pl.semaphore_signal(barrier, inc=1, device_id={"tp": neighbour}, device_id_type=pl.DeviceIdType.MESH)
    pl.semaphore_wait(barrier, 2)

    def send(k, src, dst, to):
        return pltpu.make_async_remote_copy(
            src_ref=src,
            dst_ref=dst,
            send_sem=send_sem.at[k],
            recv_sem=recv_sem.at[k],
            device_id={"tp": to},
            device_id_type=pl.DeviceIdType.MESH,
        )

    up, down = pl.ds(0, half), pl.ds(half, half)
    sends = [
        send(0, dy.at[up], dy_buf.at[1, up], right),
        send(1, dy.at[down], dy_buf.at[1, down], left),
        send(2, dy.at[down], dy_buf.at[2, up], right),
        send(3, dy.at[up], dy_buf.at[2, down], left),
        send(4, dy_buf.at[1, up], dy_buf.at[3, up], right),
        send(5, dy_buf.at[1, down], dy_buf.at[3, down], left),
        send(6, x_a, x_la, right),
        send(7, x_b, x_rb, left),
    ]
    for k in range(4):
        sends[k].start()

    def columns(j):
        return pl.ds(pl.multiple_of(j * block, block), block)

    def whole_copy(j):
        return pltpu.make_async_copy(w_down.at[pl.ds(pl.multiple_of(j * piece, piece), piece)], w_all.at[j], all_sem.at[j])

    def w_start(b):
        at = lax.rem(b, pieces) * piece
        slot = lax.rem(b, slots)
        few = piece // 4
        for c in range(4):
            src = w_in.at[pl.ds(pl.multiple_of(at + c * few, few), few)]
            pltpu.make_async_copy(src, w_buf.at[slot, pl.ds(c * few, few)], w_sem.at[slot]).start()

    def w_wait(b):
        slot = lax.rem(b, slots)
        pltpu.make_async_copy(w_in.at[pl.ds(0, piece)], w_buf.at[slot], w_sem.at[slot]).wait()

    first_rows = [
        (2 * me, 2 * me + 1),
        (2 * left, 2 * right + 1),
        (2 * left + 1, 2 * right),
        (2 * far, 2 * far + 1),
    ]

    def pre_copies(s, j):
        slot = lax.rem(j, 2)
        return [
            pltpu.make_async_copy(
                pre.at[pl.ds(pl.multiple_of(first_rows[s][k] * half, half), half), columns(j)],
                pre_buf.at[slot, pl.ds(k * half, half)],
                pre_sem.at[slot, k],
            )
            for k in range(2)
        ]

    def hid_copy(s, j):
        return pltpu.make_async_copy(hid_buf, hid.at[columns(j), pl.ds(s * rows, rows)], hid_sem)

    def narrow(j):
        return pl.ds(pl.multiple_of(j * piece, piece), piece)

    def x_copy(j):
        slot = lax.rem(j, 2)
        return pltpu.make_async_copy(x.at[:, narrow(j)], x_buf.at[slot], x_sem.at[slot])

    def turn_copies(j):
        slot = lax.rem(j, 2)
        part = hid_buf.at[pl.ds(pl.multiple_of(slot * piece, piece), piece)]
        return [
            pltpu.make_async_copy(part.at[:, up], x_a.at[narrow(j)], turn_sem.at[slot, 0]),
            pltpu.make_async_copy(part.at[:, down], x_b.at[narrow(j)], turn_sem.at[slot, 1]),
        ]

    outs_of = [(own,), (p_la, p_rb), (p_lb, p_ra), (p_oa, p_ob)]

    def out_copies(s, j):
        slot = lax.rem(j, 2)
        buf = out_wide if s % 2 == 0 else out_slim
        at, copies = 0, []
        for k, o in enumerate(outs_of[s]):
            copies.append(pltpu.make_async_copy(buf.at[slot, pl.ds(at, o.shape[0])], o.at[:, narrow(j)], out_sem.at[slot, k]))
            at += o.shape[0]
        return copies

    own_copy = pltpu.make_async_copy(dy, dy_buf.at[0], own_sem)
    own_copy.start()
    for copy in pre_copies(0, 0):
        copy.start()
    for j in range(pieces):
        whole_copy(j).start()
    for j in range(2):
        x_copy(j).start()
    own_copy.wait()

    for s in range(4):
        if s > 0:
            for k in (2 * s - 2, 2 * s - 1):
                sends[k].wait_recv()
            if s == 1:
                for k in range(4, 8):
                    sends[k].start()
            keep = pltpu.make_async_copy(dy_buf.at[s], dy_all.at[pl.ds((s - 1) * rows, rows)], dy_sem.at[s - 1])
            keep.start()

        def first(j, _, s=s):
            slot = lax.rem(j, 2)

            @pl.when(j + 1 < steps)
            def _():
                for copy in pre_copies(s, j + 1):
                    copy.start()

            if s == 0:
                for c in range(2):
                    whole_copy(2 * j + c).wait()

                @pl.when(2 * j + slots >= pieces)
                def _():
                    for c in range(2):
                        w_start(2 * j + c + slots - pieces)

            for copy in pre_copies(s, j):
                copy.wait()

            @pl.when(j >= 1)
            def _():
                hid_copy(s, j - 1).wait()

            for c in range(2):
                d_hid = nt(dy_buf[s], w_all[2 * j + c])
                h, slope = gelu_and_slope(pre_buf[slot, :, c * piece : (c + 1) * piece].astype(F32))
                hid_buf[c * piece : (c + 1) * piece, :] = h.T.astype(BF16)
                d_buf[:, pl.ds(pl.multiple_of(j * block + c * piece, piece), piece)] = (d_hid * slope).astype(BF16)
            hid_copy(s, j).start()
            return 0

        lax.fori_loop(0, steps, first, 0)
        d_copy = pltpu.make_async_copy(d_buf, d_pre.at[pl.ds(s * rows, rows)], d_sem)
        d_copy.start()
        if s < 3:
            for copy in pre_copies(s + 1, 0):
                copy.start()
        hid_copy(s, steps - 1).wait()

        def second(j, _, s=s):
            b = s * pieces + j
            slot = lax.rem(j, 2)
            if s == 0:
                x_copy(j).wait()
            w_wait(b)

            @pl.when(j >= 2)
            def _():
                for copy in out_copies(s, j - 2):
                    copy.wait()
                if s == 0:
                    for copy in turn_copies(j - 2):
                        copy.wait()

            buf = out_wide if s % 2 == 0 else out_slim
            buf[slot] = nt(d_buf[...], w_buf[lax.rem(b, slots)]).astype(buf.dtype)
            if s == 0:
                hid_buf[pl.ds(pl.multiple_of(slot * piece, piece), piece), :] = x_buf[slot].T
                for copy in turn_copies(j):
                    copy.start()

                @pl.when(j + 2 < pieces)
                def _():
                    x_copy(j + 2).start()

            for copy in out_copies(s, j):
                copy.start()

            @pl.when(b + slots < total)
            def _():
                w_start(b + slots)

            return 0

        lax.fori_loop(0, pieces, second, 0)
        for j in (pieces - 2, pieces - 1):
            for copy in out_copies(s, j):
                copy.wait()
            if s == 0:
                for copy in turn_copies(j):
                    copy.wait()
        d_copy.wait()
        if s > 0:
            keep.wait()

    for k in (6, 7):
        sends[k].wait_recv()
    for k in range(8):
        sends[k].wait_send()


def front(n, x, dy, pre, w_in, w_down):
    rows, d = dy.shape
    tokens, ff = pre.shape
    half, piece, slots = rows // 2, 512, 4
    pieces, block = ff // piece, 2 * piece
    anywhere = pl.BlockSpec(memory_space=pl.ANY)
    dma = pltpu.SemaphoreType.DMA
    shapes = [((ff, tokens), BF16), ((tokens, ff), BF16), ((tokens - rows, d), BF16)]
    shapes += [((d, half), BF16)] * 4 + [((rows, d), F32)]
    shapes += [((half, d), BF16)] * 2 + [((half, d), F32)] * 2 + [((half, d), BF16)] * 2
    out_shape = [jax.ShapeDtypeStruct(*t) for t in shapes]
    return pl.pallas_call(
        functools.partial(front_kernel, n),
        in_specs=[anywhere] * 5,
        out_specs=[anywhere] * len(out_shape),
        scratch_shapes=[
            pltpu.VMEM((4, rows, d), BF16),
            pltpu.VMEM((pieces, piece, d), BF16),
            pltpu.VMEM((slots, piece, ff), BF16),
            pltpu.VMEM((2, rows, block), BF16),
            pltpu.VMEM((2, rows, piece), BF16),
            pltpu.VMEM((rows, ff), BF16),
            pltpu.VMEM((block, rows), BF16),
            pltpu.VMEM((2, rows, piece), F32),
            pltpu.VMEM((2, rows, piece), BF16),
            dma((8,)),
            dma((8,)),
            dma,
            dma((pieces,)),
            dma((slots,)),
            dma((2, 2)),
            dma,
            dma,
            dma((2, 2)),
            dma((3,)),
            dma((2,)),
            dma((2, 2)),
        ],
        out_shape=out_shape,
        compiler_params=pltpu.CompilerParams(collective_id=0, has_side_effects=True, vmem_limit_bytes=67043328),
        cost_estimate=cost(4 * tokens * ff * d, 10 * ff * d),
        name="front",
    )(x, dy, pre, w_in, w_down)


def dw_kernel(n_lhs, n_rhs, *refs):
    lhs = [r[...] for r in refs[:n_lhs]]
    rhs = [r[...] for r in refs[n_lhs : n_lhs + n_rhs]]
    lhs = lhs[0] if n_lhs == 1 else jnp.concatenate(lhs, axis=1)
    rhs = rhs[0] if n_rhs == 1 else jnp.concatenate(rhs, axis=0)
    refs[-1][...] = jnp.dot(lhs, rhs, preferred_element_type=F32).astype(BF16)


def dw_of(lhs, rhs, room, part=0, parts=1, into=None):
    m, n = lhs[0].shape[0], rhs[0].shape[1]
    k = sum(t.shape[0] for t in rhs)
    bm, bn = min(1024, m // parts), min(2048, n)
    steps = m // parts // bm
    first = part * steps
    more = [] if into is None else [into]
    return pl.pallas_call(
        functools.partial(dw_kernel, len(lhs), len(rhs)),
        grid=(steps, n // bn),
        in_specs=[pl.BlockSpec((bm, t.shape[1]), lambda i, j: (first + i, 0)) for t in lhs]
        + [pl.BlockSpec((t.shape[0], bn), lambda i, j: (0, j)) for t in rhs]
        + [pl.BlockSpec(memory_space=pl.ANY) for _ in more],
        out_specs=pl.BlockSpec((bm, bn), lambda i, j: (first + i, j)),
        out_shape=jax.ShapeDtypeStruct((m, n), BF16),
        input_output_aliases={len(lhs) + len(rhs): 0} if more else {},
        compiler_params=pltpu.CompilerParams(vmem_limit_bytes=room << 20),
        cost_estimate=cost(2 * m * n * k // parts, 2 * m * n // parts),
    )(*lhs, *rhs, *more)


def last_kernel(sum_ref, over_left, over_right, o_ref):
    half = over_left.shape[0]
    o_ref[:half, :] = (sum_ref[:half, :] + over_left[...].astype(F32)).astype(BF16)
    o_ref[half:, :] = (sum_ref[half:, :] + over_right[...].astype(F32)).astype(BF16)


def near_kernel(own_ref, from_right, from_left, o_ref):
    half = from_left.shape[0]
    o_ref[:half, :] = own_ref[:half, :] + from_right[...].astype(F32)
    o_ref[half:, :] = own_ref[half:, :] + from_left[...].astype(F32)


def sum_of(kernel, whole, top, low, dtype):
    rows, d = whole.shape
    half, bd = rows // 2, min(1024, d)
    piece = pl.BlockSpec((half, bd), lambda j: (0, j))
    full = pl.BlockSpec((rows, bd), lambda j: (0, j))
    return pl.pallas_call(
        kernel,
        grid=(d // bd,),
        in_specs=[full, piece, piece],
        out_specs=full,
        out_shape=jax.ShapeDtypeStruct((rows, d), dtype),
        compiler_params=pltpu.CompilerParams(vmem_limit_bytes=16 << 20),
        cost_estimate=cost(rows * d * 100, rows * d * 10),
    )(whole, top, low)


def solution(mesh):
    n = mesh.shape["tp"]
    to_right = [(i, (i + 1) % n) for i in range(n)]
    to_left = [(i, (i - 1) % n) for i in range(n)]

    def right(t):
        return lax.ppermute(t, "tp", to_right)

    def left(t):
        return lax.ppermute(t, "tp", to_left)

    def step(x, dy, pre, w_in, w_down):
        (hid, d_pre, dy_all, x_la, x_rb, x_a, x_b, own, p_la, p_rb, p_lb, p_ra, p_oa, p_ob) = front(
            n, x, dy, pre, w_in, w_down
        )
        x_lb = right(x_b)
        x_ra = left(x_a)
        x_oa = right(x_la)
        x_ob = left(x_rb)

        in_l = right(p_oa)
        in_r = left(p_ob)
        from_left = right(p_rb)
        from_right = left(p_la)
        over_left = right((p_ra + in_l.astype(F32)).astype(BF16))
        over_right = left((p_lb + in_r.astype(F32)).astype(BF16))

        dw_down = dw_of([hid], [dy, dy_all], 50)
        xs = [x_a, x_b, x_la, x_rb, x_lb, x_ra, x_oa, x_ob]
        dw_in = dw_of(xs, [d_pre], 28, 0, 2)
        dw_in = dw_of(xs, [d_pre], 28, 1, 2, dw_in)
        near = sum_of(near_kernel, own, from_right, from_left, F32)
        dx = sum_of(last_kernel, near, over_left, over_right, BF16)
        return dx, dw_in, dw_down

    return jax.shard_map(
        step,
        mesh=mesh,
        in_specs=(P(("dp", "tp"), None), P(("dp", "tp"), None), P("dp", "tp"), P(None, "tp"), P("tp", None)),
        out_specs=(P(("dp", "tp"), None), P("dp", "tp"), P(("dp", "tp"), None)),
        check_vma=False,
    )
```

```python
import functools

import jax
import jax.numpy as jnp
from jax import lax
from jax.experimental import pallas as pl
from jax.experimental.pallas import tpu as pltpu
from jax.sharding import PartitionSpec as P


F32, BF16 = jnp.float32, jnp.bfloat16

C0 = 0.7978845608028654
C1 = 0.044715


def nt(a, b):
    return lax.dot_general(a, b, (((1,), (1,)), ((), ())), preferred_element_type=F32)


def cost(flops, nbytes):
    return pl.CostEstimate(flops=int(flops), bytes_accessed=int(nbytes), transcendentals=0)


def gelu_and_slope(x):
    xx = x * x
    t = jnp.tanh(x * (C0 + (C0 * C1) * xx))
    cdf = 0.5 + 0.5 * t
    return x * cdf, cdf + (0.5 * ((1.0 - t * t) * x)) * (C0 + (3.0 * C0 * C1) * xx)


def front_kernel(n, x, dy, pre, w_in, w_down, hid, d_pre, dy_all, x_la, x_rb, x_a, x_b, own, p_la, p_rb, p_lb, p_ra, p_oa, p_ob, *scratch):
    dy_buf, w_all, w_buf, pre_buf, x_buf, d_buf, hid_buf, turn_buf, out_wide, out_slim = scratch[:10]
    send_sem, recv_sem, own_sem, all_sem, w_sem, pre_sem, d_sem, hid_sem, out_sem, dy_sem, x_sem, turn_sem = scratch[10:]
    me = lax.axis_index("tp")
    right, left, far = lax.rem(me + 1, n), lax.rem(me + n - 1, n), lax.rem(me + 2, n)
    pieces, piece, _ = w_all.shape
    slots = w_buf.shape[0]
    block = 2 * piece
    steps = pieces // 2
    rows = dy.shape[0]
    half = rows // 2
    total = 4 * pieces

    barrier = pltpu.get_barrier_semaphore()
    for neighbour in (left, right):
        pl.semaphore_signal(barrier, inc=1, device_id={"tp": neighbour}, device_id_type=pl.DeviceIdType.MESH)
    pl.semaphore_wait(barrier, 2)

    def send(k, src, dst, to):
        return pltpu.make_async_remote_copy(
            src_ref=src,
            dst_ref=dst,
            send_sem=send_sem.at[k],
            recv_sem=recv_sem.at[k],
            device_id={"tp": to},
            device_id_type=pl.DeviceIdType.MESH,
        )

    up, down = pl.ds(0, half), pl.ds(half, half)
    sends = [
        send(0, dy.at[up], dy_buf.at[1, up], right),
        send(1, dy.at[down], dy_buf.at[1, down], left),
        send(2, dy.at[down], dy_buf.at[2, up], right),
        send(3, dy.at[up], dy_buf.at[2, down], left),
        send(4, dy_buf.at[1, up], dy_buf.at[3, up], right),
        send(5, dy_buf.at[1, down], dy_buf.at[3, down], left),
        send(6, x_a, x_la, right),
        send(7, x_b, x_rb, left),
    ]
    for k in range(4):
        sends[k].start()

    def columns(j):
        return pl.ds(pl.multiple_of(j * block, block), block)

    def whole_copy(j):
        return pltpu.make_async_copy(w_down.at[pl.ds(pl.multiple_of(j * piece, piece), piece)], w_all.at[j], all_sem.at[j])

    def w_start(b):
        at = lax.rem(b, pieces) * piece
        slot = lax.rem(b, slots)
        few = piece // 4
        for c in range(4):
            src = w_in.at[pl.ds(pl.multiple_of(at + c * few, few), few)]
            pltpu.make_async_copy(src, w_buf.at[slot, pl.ds(c * few, few)], w_sem.at[slot]).start()

    def w_wait(b):
        slot = lax.rem(b, slots)
        pltpu.make_async_copy(w_in.at[pl.ds(0, piece)], w_buf.at[slot], w_sem.at[slot]).wait()

    first_rows = [
        (2 * me, 2 * me + 1),
        (2 * left, 2 * right + 1),
        (2 * left + 1, 2 * right),
        (2 * far, 2 * far + 1),
    ]

    def pre_copies(s, j):
        slot = lax.rem(j, 2)
        return [
            pltpu.make_async_copy(
                pre.at[pl.ds(pl.multiple_of(first_rows[s][k] * half, half), half), columns(j)],
                pre_buf.at[slot, pl.ds(k * half, half)],
                pre_sem.at[slot, k],
            )
            for k in range(2)
        ]

    def hid_copy(s, j):
        slot = lax.rem(j, 2)
        return pltpu.make_async_copy(hid_buf.at[slot], hid.at[columns(j), pl.ds(s * rows, rows)], hid_sem.at[slot])

    def narrow(j):
        return pl.ds(pl.multiple_of(j * piece, piece), piece)

    def x_copy(j):
        slot = lax.rem(j, 2)
        return pltpu.make_async_copy(x.at[:, narrow(j)], x_buf.at[slot], x_sem.at[slot])

    def turn_copies(j):
        slot = lax.rem(j, 2)
        return [
            pltpu.make_async_copy(turn_buf.at[slot, :, up], x_a.at[narrow(j)], turn_sem.at[slot, 0]),
            pltpu.make_async_copy(turn_buf.at[slot, :, down], x_b.at[narrow(j)], turn_sem.at[slot, 1]),
        ]

    outs_of = [(own,), (p_la, p_rb), (p_lb, p_ra), (p_oa, p_ob)]

    def out_copies(s, j):
        slot = lax.rem(j, 2)
        buf = out_wide if s % 2 == 0 else out_slim
        at, copies = 0, []
        for k, o in enumerate(outs_of[s]):
            copies.append(pltpu.make_async_copy(buf.at[slot, pl.ds(at, o.shape[0])], o.at[:, narrow(j)], out_sem.at[slot, k]))
            at += o.shape[0]
        return copies

    own_copy = pltpu.make_async_copy(dy, dy_buf.at[0], own_sem)
    own_copy.start()
    for copy in pre_copies(0, 0):
        copy.start()
    for j in range(pieces):
        whole_copy(j).start()
    for j in range(2):
        x_copy(j).start()
    own_copy.wait()

    for s in range(4):
        if s > 0:
            for k in (2 * s - 2, 2 * s - 1):
                sends[k].wait_recv()
            if s == 1:
                for k in range(4, 8):
                    sends[k].start()
            keep = pltpu.make_async_copy(dy_buf.at[s], dy_all.at[pl.ds((s - 1) * rows, rows)], dy_sem.at[s - 1])
            keep.start()

        def first(j, _, s=s):
            slot = lax.rem(j, 2)

            @pl.when(j + 1 < steps)
            def _():
                for copy in pre_copies(s, j + 1):
                    copy.start()

            if s == 0:
                for c in range(2):
                    whole_copy(2 * j + c).wait()

                for c in range(2):

                    @pl.when(2 * j + c + slots >= pieces)
                    def _(c=c):
                        w_start(2 * j + c + slots - pieces)

            for copy in pre_copies(s, j):
                copy.wait()

            @pl.when(j >= 2)
            def _():
                hid_copy(s, j - 2).wait()

            for c in range(2):
                d_hid = nt(dy_buf[s], w_all[2 * j + c])
                h, slope = gelu_and_slope(pre_buf[slot, :, c * piece : (c + 1) * piece].astype(F32))
                hid_buf[slot, c * piece : (c + 1) * piece, :] = h.T.astype(BF16)
                d_buf[:, pl.ds(pl.multiple_of(j * block + c * piece, piece), piece)] = (d_hid * slope).astype(BF16)
            hid_copy(s, j).start()
            return 0

        lax.fori_loop(0, steps, first, 0)
        d_copy = pltpu.make_async_copy(d_buf, d_pre.at[pl.ds(s * rows, rows)], d_sem)
        d_copy.start()
        if s < 3:
            for copy in pre_copies(s + 1, 0):
                copy.start()

        def second(j, _, s=s):
            b = s * pieces + j
            slot = lax.rem(j, 2)
            if s == 0:
                x_copy(j).wait()
            w_wait(b)

            @pl.when(j >= 2)
            def _():
                for copy in out_copies(s, j - 2):
                    copy.wait()
                if s == 0:
                    for copy in turn_copies(j - 2):
                        copy.wait()

            buf = out_wide if s % 2 == 0 else out_slim
            buf[slot] = nt(d_buf[...], w_buf[lax.rem(b, slots)]).astype(buf.dtype)
            if s == 0:
                turn_buf[slot] = x_buf[slot].T
                for copy in turn_copies(j):
                    copy.start()

                @pl.when(j + 2 < pieces)
                def _():
                    x_copy(j + 2).start()

            for copy in out_copies(s, j):
                copy.start()

            @pl.when(b + slots < total)
            def _():
                w_start(b + slots)

            return 0

        lax.fori_loop(0, pieces, second, 0)
        for j in (pieces - 2, pieces - 1):
            for copy in out_copies(s, j):
                copy.wait()
            if s == 0:
                for copy in turn_copies(j):
                    copy.wait()
        d_copy.wait()
        for j in (steps - 2, steps - 1):
            hid_copy(s, j).wait()
        if s > 0:
            keep.wait()

    for k in (6, 7):
        sends[k].wait_recv()
    for k in range(8):
        sends[k].wait_send()


def front(n, x, dy, pre, w_in, w_down):
    rows, d = dy.shape
    tokens, ff = pre.shape
    half, piece, slots = rows // 2, 512, 3
    pieces, block = ff // piece, 2 * piece
    anywhere = pl.BlockSpec(memory_space=pl.ANY)
    dma = pltpu.SemaphoreType.DMA
    shapes = [((ff, tokens), BF16), ((tokens, ff), BF16), ((tokens - rows, d), BF16)]
    shapes += [((d, half), BF16)] * 4 + [((rows, d), F32)]
    shapes += [((half, d), BF16)] * 2 + [((half, d), F32)] * 2 + [((half, d), BF16)] * 2
    out_shape = [jax.ShapeDtypeStruct(*t) for t in shapes]
    return pl.pallas_call(
        functools.partial(front_kernel, n),
        in_specs=[anywhere] * 5,
        out_specs=[anywhere] * len(out_shape),
        scratch_shapes=[
            pltpu.VMEM((4, rows, d), BF16),
            pltpu.VMEM((pieces, piece, d), BF16),
            pltpu.VMEM((slots, piece, ff), BF16),
            pltpu.VMEM((2, rows, block), BF16),
            pltpu.VMEM((2, rows, piece), BF16),
            pltpu.VMEM((rows, ff), BF16),
            pltpu.VMEM((2, block, rows), BF16),
            pltpu.VMEM((2, piece, rows), BF16),
            pltpu.VMEM((2, rows, piece), F32),
            pltpu.VMEM((2, rows, piece), BF16),
            dma((8,)),
            dma((8,)),
            dma,
            dma((pieces,)),
            dma((slots,)),
            dma((2, 2)),
            dma,
            dma((2,)),
            dma((2, 2)),
            dma((3,)),
            dma((2,)),
            dma((2, 2)),
        ],
        out_shape=out_shape,
        compiler_params=pltpu.CompilerParams(collective_id=0, has_side_effects=True, vmem_limit_bytes=67043328),
        cost_estimate=cost(4 * tokens * ff * d, 10 * ff * d),
        name="front",
    )(x, dy, pre, w_in, w_down)


def dw_kernel(n_lhs, n_rhs, *refs):
    lhs = [r[...] for r in refs[:n_lhs]]
    rhs = [r[...] for r in refs[n_lhs : n_lhs + n_rhs]]
    lhs = lhs[0] if n_lhs == 1 else jnp.concatenate(lhs, axis=1)
    rhs = rhs[0] if n_rhs == 1 else jnp.concatenate(rhs, axis=0)
    refs[-1][...] = jnp.dot(lhs, rhs, preferred_element_type=F32).astype(BF16)


def dw_of(lhs, rhs, room, part=0, parts=1, into=None):
    m, n = lhs[0].shape[0], rhs[0].shape[1]
    k = sum(t.shape[0] for t in rhs)
    bm, bn = min(1024, m // parts), min(2048, n)
    steps = m // parts // bm
    first = part * steps
    more = [] if into is None else [into]
    return pl.pallas_call(
        functools.partial(dw_kernel, len(lhs), len(rhs)),
        grid=(steps, n // bn),
        in_specs=[pl.BlockSpec((bm, t.shape[1]), lambda i, j: (first + i, 0)) for t in lhs]
        + [pl.BlockSpec((t.shape[0], bn), lambda i, j: (0, j)) for t in rhs]
        + [pl.BlockSpec(memory_space=pl.ANY) for _ in more],
        out_specs=pl.BlockSpec((bm, bn), lambda i, j: (first + i, j)),
        out_shape=jax.ShapeDtypeStruct((m, n), BF16),
        input_output_aliases={len(lhs) + len(rhs): 0} if more else {},
        compiler_params=pltpu.CompilerParams(vmem_limit_bytes=room << 20),
        cost_estimate=cost(2 * m * n * k // parts, 2 * m * n // parts),
    )(*lhs, *rhs, *more)


def last_kernel(sum_ref, over_left, over_right, o_ref):
    half = over_left.shape[0]
    o_ref[:half, :] = (sum_ref[:half, :] + over_left[...].astype(F32)).astype(BF16)
    o_ref[half:, :] = (sum_ref[half:, :] + over_right[...].astype(F32)).astype(BF16)


def near_kernel(own_ref, from_right, from_left, o_ref):
    half = from_left.shape[0]
    o_ref[:half, :] = own_ref[:half, :] + from_right[...].astype(F32)
    o_ref[half:, :] = own_ref[half:, :] + from_left[...].astype(F32)


def sum_of(kernel, whole, top, low, dtype):
    rows, d = whole.shape
    half, bd = rows // 2, min(1024, d)
    piece = pl.BlockSpec((half, bd), lambda j: (0, j))
    full = pl.BlockSpec((rows, bd), lambda j: (0, j))
    return pl.pallas_call(
        kernel,
        grid=(d // bd,),
        in_specs=[full, piece, piece],
        out_specs=full,
        out_shape=jax.ShapeDtypeStruct((rows, d), dtype),
        compiler_params=pltpu.CompilerParams(vmem_limit_bytes=16 << 20),
        cost_estimate=cost(rows * d * 100, rows * d * 10),
    )(whole, top, low)


def solution(mesh):
    n = mesh.shape["tp"]
    to_right = [(i, (i + 1) % n) for i in range(n)]
    to_left = [(i, (i - 1) % n) for i in range(n)]

    def right(t):
        return lax.ppermute(t, "tp", to_right)

    def left(t):
        return lax.ppermute(t, "tp", to_left)

    def step(x, dy, pre, w_in, w_down):
        (hid, d_pre, dy_all, x_la, x_rb, x_a, x_b, own, p_la, p_rb, p_lb, p_ra, p_oa, p_ob) = front(
            n, x, dy, pre, w_in, w_down
        )
        x_lb = right(x_b)
        x_ra = left(x_a)
        x_oa = right(x_la)
        x_ob = left(x_rb)

        in_l = right(p_oa)
        in_r = left(p_ob)
        from_left = right(p_rb)
        from_right = left(p_la)
        over_left = right((p_ra + in_l.astype(F32)).astype(BF16))
        over_right = left((p_lb + in_r.astype(F32)).astype(BF16))

        dw_down = dw_of([hid], [dy, dy_all], 50)
        xs = [x_a, x_b, x_la, x_rb, x_lb, x_ra, x_oa, x_ob]
        dw_in = dw_of(xs, [d_pre], 28, 0, 2)
        dw_in = dw_of(xs, [d_pre], 28, 1, 2, dw_in)
        near = sum_of(near_kernel, own, from_right, from_left, F32)
        dx = sum_of(last_kernel, near, over_left, over_right, BF16)
        return dx, dw_in, dw_down

    return jax.shard_map(
        step,
        mesh=mesh,
        in_specs=(P(("dp", "tp"), None), P(("dp", "tp"), None), P("dp", "tp"), P(None, "tp"), P("tp", None)),
        out_specs=(P(("dp", "tp"), None), P("dp", "tp"), P(("dp", "tp"), None)),
        check_vma=False,
    )
```

```python
import functools

import jax
import jax.numpy as jnp
from jax import lax
from jax.experimental import pallas as pl
from jax.experimental.pallas import tpu as pltpu
from jax.sharding import PartitionSpec as P


F32, BF16 = jnp.float32, jnp.bfloat16

C0 = 0.7978845608028654
C1 = 0.044715


def nt(a, b):
    return lax.dot_general(a, b, (((1,), (1,)), ((), ())), preferred_element_type=F32)


def cost(flops, nbytes):
    return pl.CostEstimate(flops=int(flops), bytes_accessed=int(nbytes), transcendentals=0)


def gelu_and_slope(x):
    xx = x * x
    t = jnp.tanh(x * (C0 + (C0 * C1) * xx))
    cdf = 0.5 + 0.5 * t
    return x * cdf, cdf + (0.5 * ((1.0 - t * t) * x)) * (C0 + (3.0 * C0 * C1) * xx)


def front_kernel(n, x, dy, pre, w_in, w_down, hid, d_pre, dy_all, x_la, x_rb, x_a1, x_a2, x_b1, x_b2, x_lb1, x_ra1, own, p_la, p_rb, p_lb, p_ra, p_oa, p_ob, *scratch):
    dy_buf, w_all, w_buf, pre_buf, x_buf, d_buf, hid_buf, turn_buf, out_wide, out_slim = scratch[:10]
    send_sem, recv_sem, own_sem, all_sem, w_sem, pre_sem, d_sem, hid_sem, out_sem, dy_sem, x_sem, turn_sem = scratch[10:]
    me = lax.axis_index("tp")
    right, left, far = lax.rem(me + 1, n), lax.rem(me + n - 1, n), lax.rem(me + 2, n)
    pieces, piece, _ = w_all.shape
    slots = w_buf.shape[0]
    block = 2 * piece
    steps = pieces // 2
    rows = dy.shape[0]
    half = rows // 2
    total = 4 * pieces

    barrier = pltpu.get_barrier_semaphore()
    for neighbour in (left, right):
        pl.semaphore_signal(barrier, inc=1, device_id={"tp": neighbour}, device_id_type=pl.DeviceIdType.MESH)

    def send(k, src, dst, to):
        return pltpu.make_async_remote_copy(
            src_ref=src,
            dst_ref=dst,
            send_sem=send_sem.at[k],
            recv_sem=recv_sem.at[k],
            device_id={"tp": to},
            device_id_type=pl.DeviceIdType.MESH,
        )

    up, down = pl.ds(0, half), pl.ds(half, half)
    first_part, second_part = pl.ds(0, x_a1.shape[0]), pl.ds(x_a1.shape[0], x_a2.shape[0])
    sends = [
        send(0, dy.at[up], dy_buf.at[1, up], right),
        send(1, dy.at[down], dy_buf.at[1, down], left),
        send(2, dy.at[down], dy_buf.at[2, up], right),
        send(3, dy.at[up], dy_buf.at[2, down], left),
        send(4, dy_buf.at[1, up], dy_buf.at[3, up], right),
        send(5, dy_buf.at[1, down], dy_buf.at[3, down], left),
        send(6, x_a1, x_la.at[first_part], right),
        send(7, x_b1, x_rb.at[first_part], left),
        send(8, x_a2, x_la.at[second_part], right),
        send(9, x_b2, x_rb.at[second_part], left),
        send(10, x_b1, x_lb1, right),
        send(11, x_a1, x_ra1, left),
    ]

    def columns(j):
        return pl.ds(pl.multiple_of(j * block, block), block)

    def whole_copy(j):
        return pltpu.make_async_copy(w_down.at[pl.ds(pl.multiple_of(j * piece, piece), piece)], w_all.at[j], all_sem.at[j])

    def w_start(b):
        at = lax.rem(b, pieces) * piece
        slot = lax.rem(b, slots)
        few = piece // 4
        for c in range(4):
            src = w_in.at[pl.ds(pl.multiple_of(at + c * few, few), few)]
            pltpu.make_async_copy(src, w_buf.at[slot, pl.ds(c * few, few)], w_sem.at[slot]).start()

    def w_wait(b):
        slot = lax.rem(b, slots)
        pltpu.make_async_copy(w_in.at[pl.ds(0, piece)], w_buf.at[slot], w_sem.at[slot]).wait()

    first_rows = [
        (2 * me, 2 * me + 1),
        (2 * left, 2 * right + 1),
        (2 * left + 1, 2 * right),
        (2 * far, 2 * far + 1),
    ]

    def pre_copies(s, j):
        slot = lax.rem(j, 2)
        return [
            pltpu.make_async_copy(
                pre.at[pl.ds(pl.multiple_of(first_rows[s][k] * half, half), half), columns(j)],
                pre_buf.at[slot, pl.ds(k * half, half)],
                pre_sem.at[slot, k],
            )
            for k in range(2)
        ]

    def hid_copy(s, j):
        slot = lax.rem(j, 2)
        return pltpu.make_async_copy(hid_buf.at[slot], hid.at[columns(j), pl.ds(s * rows, rows)], hid_sem.at[slot])

    def narrow(j):
        return pl.ds(pl.multiple_of(j * piece, piece), piece)

    def x_copy(j):
        slot = lax.rem(j, 2)
        return pltpu.make_async_copy(x.at[:, narrow(j)], x_buf.at[slot], x_sem.at[slot])

    early = x_a1.shape[0] // piece

    def turn_start(j):
        slot = lax.rem(j, 2)

        def to(a, b, at):
            at = pl.ds(pl.multiple_of(at * piece, piece), piece)
            pltpu.make_async_copy(turn_buf.at[slot, :, up], a.at[at], turn_sem.at[slot, 0]).start()
            pltpu.make_async_copy(turn_buf.at[slot, :, down], b.at[at], turn_sem.at[slot, 1]).start()

        @pl.when(j < early)
        def _():
            to(x_a1, x_b1, j)

        @pl.when(j >= early)
        def _():
            to(x_a2, x_b2, j - early)

    def turn_wait(j):
        slot = lax.rem(j, 2)
        at = pl.ds(0, piece)
        pltpu.make_async_copy(turn_buf.at[slot, :, up], x_a1.at[at], turn_sem.at[slot, 0]).wait()
        pltpu.make_async_copy(turn_buf.at[slot, :, down], x_b1.at[at], turn_sem.at[slot, 1]).wait()

    outs_of = [(own,), (p_la, p_rb), (p_lb, p_ra), (p_oa, p_ob)]

    def out_copies(s, j):
        slot = lax.rem(j, 2)
        buf = out_wide if s % 2 == 0 else out_slim
        at, copies = 0, []
        for k, o in enumerate(outs_of[s]):
            copies.append(pltpu.make_async_copy(buf.at[slot, pl.ds(at, o.shape[0])], o.at[:, narrow(j)], out_sem.at[s % 2, slot, k]))
            at += o.shape[0]
        return copies

    own_copy = pltpu.make_async_copy(dy, dy_buf.at[0], own_sem)
    own_copy.start()
    for copy in pre_copies(0, 0):
        copy.start()
    for j in range(2):
        whole_copy(j).start()
    pl.semaphore_wait(barrier, 2)
    for k in range(4):
        sends[k].start()
    own_copy.wait()
    for j in range(2, 4):
        whole_copy(j).start()
    for j in range(2):
        x_copy(j).start()

    for s in range(4):
        if s > 0:
            for k in (2 * s - 2, 2 * s - 1):
                sends[k].wait_recv()
            if s == 1:
                for k in range(4, 6):
                    sends[k].start()
                for j in (pieces - 2, pieces - 1):
                    turn_wait(j)
                for k in range(6, 12):
                    sends[k].start()
            keep = pltpu.make_async_copy(dy_buf.at[s], dy_all.at[pl.ds((s - 1) * rows, rows)], dy_sem.at[s - 1])
            keep.start()

        def first(j, _, s=s):
            slot = lax.rem(j, 2)

            @pl.when(j + 1 < steps)
            def _():
                for copy in pre_copies(s, j + 1):
                    copy.start()

            if s == 0:
                for c in range(2):
                    whole_copy(2 * j + c).wait()

                for c in range(2):

                    @pl.when(2 * j + c + 4 < pieces)
                    def _(c=c):
                        whole_copy(2 * j + c + 4).start()

                    @pl.when(2 * j + c + slots >= pieces)
                    def _(c=c):
                        w_start(2 * j + c + slots - pieces)

            for copy in pre_copies(s, j):
                copy.wait()

            if s == 0:

                @pl.when(j >= 2)
                def _():
                    hid_copy(s, j).wait()
            else:
                hid_copy(s, j).wait()

            for c in range(2):
                d_hid = nt(dy_buf[s], w_all[2 * j + c])
                h, slope = gelu_and_slope(pre_buf[slot, :, c * piece : (c + 1) * piece].astype(F32))
                hid_buf[slot, c * piece : (c + 1) * piece, :] = h.T.astype(BF16)
                d_buf[:, pl.ds(pl.multiple_of(j * block + c * piece, piece), piece)] = (d_hid * slope).astype(BF16)
            hid_copy(s, j).start()
            return 0

        lax.fori_loop(0, steps, first, 0)
        d_copy = pltpu.make_async_copy(d_buf, d_pre.at[pl.ds(s * rows, rows)], d_sem)
        d_copy.start()
        if s > 0:
            for j in (pieces - 2, pieces - 1):
                for copy in out_copies(s - 1, j):
                    copy.wait()
        if s < 3:
            for copy in pre_copies(s + 1, 0):
                copy.start()

        def second(j, _, s=s):
            b = s * pieces + j
            slot = lax.rem(j, 2)
            if s == 0:
                x_copy(j).wait()
            w_wait(b)

            @pl.when(j >= 2)
            def _():
                for copy in out_copies(s, j - 2):
                    copy.wait()
                if s == 0:
                    turn_wait(j)

            buf = out_wide if s % 2 == 0 else out_slim
            buf[slot] = nt(d_buf[...], w_buf[lax.rem(b, slots)]).astype(buf.dtype)
            if s == 0:
                turn_buf[slot] = x_buf[slot].T
                turn_start(j)

                @pl.when(j + 2 < pieces)
                def _():
                    x_copy(j + 2).start()

            for copy in out_copies(s, j):
                copy.start()

            @pl.when(b + slots < total)
            def _():
                w_start(b + slots)

            return 0

        lax.fori_loop(0, pieces, second, 0)
        d_copy.wait()
        if s > 0:
            keep.wait()

    for j in (pieces - 2, pieces - 1):
        for copy in out_copies(3, j):
            copy.wait()
    for j in (steps - 2, steps - 1):
        hid_copy(3, j).wait()
    for k in range(6, 12):
        sends[k].wait_recv()
    for k in range(12):
        sends[k].wait_send()


def front(n, x, dy, pre, w_in, w_down):
    rows, d = dy.shape
    tokens, ff = pre.shape
    half, piece, slots = rows // 2, 512, 3
    pieces, block = ff // piece, 2 * piece
    anywhere = pl.BlockSpec(memory_space=pl.ANY)
    dma = pltpu.SemaphoreType.DMA
    shapes = [((ff, tokens), BF16), ((tokens, ff), BF16), ((tokens - rows, d), BF16)]
    shapes += [((d, half), BF16)] * 2 + [((d // 4, half), BF16), ((d - d // 4, half), BF16)] * 2
    shapes += [((d // 4, half), BF16)] * 2 + [((rows, d), F32)]
    shapes += [((half, d), BF16)] * 2 + [((half, d), F32)] * 2 + [((half, d), BF16)] * 2
    out_shape = [jax.ShapeDtypeStruct(*t) for t in shapes]
    return pl.pallas_call(
        functools.partial(front_kernel, n),
        in_specs=[anywhere] * 5,
        out_specs=[anywhere] * len(out_shape),
        scratch_shapes=[
            pltpu.VMEM((4, rows, d), BF16),
            pltpu.VMEM((pieces, piece, d), BF16),
            pltpu.VMEM((slots, piece, ff), BF16),
            pltpu.VMEM((2, rows, block), BF16),
            pltpu.VMEM((2, rows, piece), BF16),
            pltpu.VMEM((rows, ff), BF16),
            pltpu.VMEM((2, block, rows), BF16),
            pltpu.VMEM((2, piece, rows), BF16),
            pltpu.VMEM((2, rows, piece), F32),
            pltpu.VMEM((2, rows, piece), BF16),
            dma((12,)),
            dma((12,)),
            dma,
            dma((pieces,)),
            dma((slots,)),
            dma((2, 2)),
            dma,
            dma((2,)),
            dma((2, 2, 2)),
            dma((3,)),
            dma((2,)),
            dma((2, 2)),
        ],
        out_shape=out_shape,
        compiler_params=pltpu.CompilerParams(collective_id=0, has_side_effects=True, vmem_limit_bytes=67043328),
        cost_estimate=cost(4 * tokens * ff * d, 10 * ff * d),
        name="front",
    )(x, dy, pre, w_in, w_down)


def dw_kernel(n_lhs, n_rhs, *refs):
    lhs = [r[...] for r in refs[:n_lhs]]
    rhs = [r[...] for r in refs[n_lhs : n_lhs + n_rhs]]
    lhs = lhs[0] if n_lhs == 1 else jnp.concatenate(lhs, axis=1)
    rhs = rhs[0] if n_rhs == 1 else jnp.concatenate(rhs, axis=0)
    refs[-1][...] = jnp.dot(lhs, rhs, preferred_element_type=F32).astype(BF16)


def dw_of(lhs, rhs, room, rows=None, into=None):
    m, n = max(t.shape[0] for t in lhs), rhs[0].shape[1]
    low, high = rows or (0, m)
    k = sum(t.shape[0] for t in rhs)
    bm, bn = min(1024, high - low), min(2048, n)
    first = low // bm
    more = [] if into is None else [into]

    def at(t):
        return first if t.shape[0] == m else 0

    return pl.pallas_call(
        functools.partial(dw_kernel, len(lhs), len(rhs)),
        grid=((high - low) // bm, n // bn),
        in_specs=[pl.BlockSpec((bm, t.shape[1]), lambda i, j, s=at(t): (s + i, 0)) for t in lhs]
        + [pl.BlockSpec((t.shape[0], bn), lambda i, j: (0, j)) for t in rhs]
        + [pl.BlockSpec(memory_space=pl.ANY) for _ in more],
        out_specs=pl.BlockSpec((bm, bn), lambda i, j: (first + i, j)),
        out_shape=jax.ShapeDtypeStruct((m, n), BF16),
        input_output_aliases={len(lhs) + len(rhs): 0} if more else {},
        compiler_params=pltpu.CompilerParams(vmem_limit_bytes=room << 20),
        cost_estimate=cost(2 * (high - low) * n * k, 2 * (high - low) * n),
    )(*lhs, *rhs, *more)


def last_kernel(sum_ref, over_ref, *refs):
    refs[-1][...] = (sum_ref[...] + over_ref[...].astype(F32)).astype(BF16)


def last_sum(whole, over, at, into=None):
    rows, d = whole.shape
    half, bd = rows // 2, min(1024, d)
    more = [] if into is None else [into]
    part = pl.BlockSpec((half, bd), lambda j: (at, j))
    return pl.pallas_call(
        last_kernel,
        grid=(d // bd,),
        in_specs=[part, pl.BlockSpec((half, bd), lambda j: (0, j))] + [pl.BlockSpec(memory_space=pl.ANY) for _ in more],
        out_specs=part,
        out_shape=jax.ShapeDtypeStruct((rows, d), BF16),
        input_output_aliases={2: 0} if more else {},
        compiler_params=pltpu.CompilerParams(vmem_limit_bytes=16 << 20),
        cost_estimate=cost(half * d * 100, half * d * 8),
    )(whole, over, *more)


def near_kernel(own_ref, from_right, from_left, o_ref):
    half = from_left.shape[0]
    o_ref[:half, :] = own_ref[:half, :] + from_right[...].astype(F32)
    o_ref[half:, :] = own_ref[half:, :] + from_left[...].astype(F32)


def sum_of(kernel, whole, top, low, dtype):
    rows, d = whole.shape
    half, bd = rows // 2, min(1024, d)
    piece = pl.BlockSpec((half, bd), lambda j: (0, j))
    full = pl.BlockSpec((rows, bd), lambda j: (0, j))
    return pl.pallas_call(
        kernel,
        grid=(d // bd,),
        in_specs=[full, piece, piece],
        out_specs=full,
        out_shape=jax.ShapeDtypeStruct((rows, d), dtype),
        compiler_params=pltpu.CompilerParams(vmem_limit_bytes=16 << 20),
        cost_estimate=cost(rows * d * 100, rows * d * 10),
    )(whole, top, low)


def solution(mesh):
    n = mesh.shape["tp"]
    to_right = [(i, (i + 1) % n) for i in range(n)]
    to_left = [(i, (i - 1) % n) for i in range(n)]

    def right(t):
        return lax.ppermute(t, "tp", to_right)

    def left(t):
        return lax.ppermute(t, "tp", to_left)

    def step(x, dy, pre, w_in, w_down):
        (hid, d_pre, dy_all, x_la, x_rb, x_a1, x_a2, x_b1, x_b2, x_lb1, x_ra1, own, *parts) = front(
            n, x, dy, pre, w_in, w_down
        )
        p_la, p_rb, p_lb, p_ra, p_oa, p_ob = parts
        x_lb2 = right(x_b2)
        x_ra2 = left(x_a2)
        x_oa = right(x_la)
        x_ob = left(x_rb)

        in_l = right(p_oa)
        in_r = left(p_ob)
        from_left = right(p_rb)
        from_right = left(p_la)
        over_left = right((p_ra + in_l.astype(F32)).astype(BF16))
        over_right = left((p_lb + in_r.astype(F32)).astype(BF16))

        dw_down = dw_of([hid], [dy, dy_all], 52)
        d, cut = x_la.shape[0], x_a1.shape[0]
        xs = [x_a1, x_b1, x_la, x_rb, x_lb1, x_ra1, x_oa, x_ob]
        dw_in = dw_of(xs, [d_pre], 28, (0, cut))
        xs = [x_a2, x_b2, x_la, x_rb, x_lb2, x_ra2, x_oa, x_ob]
        dw_in = dw_of(xs, [d_pre], 28, (cut, d), dw_in)
        near = sum_of(near_kernel, own, from_right, from_left, F32)
        dx = last_sum(near, over_left, 0)
        dx = last_sum(near, over_right, 1, dx)
        return dx, dw_in, dw_down

    return jax.shard_map(
        step,
        mesh=mesh,
        in_specs=(P(("dp", "tp"), None), P(("dp", "tp"), None), P("dp", "tp"), P(None, "tp"), P("tp", None)),
        out_specs=(P(("dp", "tp"), None), P("dp", "tp"), P(("dp", "tp"), None)),
        check_vma=False,
    )
```

```python
import functools

import jax
import jax.numpy as jnp
from jax import lax
from jax.experimental import pallas as pl
from jax.experimental.pallas import tpu as pltpu
from jax.sharding import PartitionSpec as P


F32, BF16 = jnp.float32, jnp.bfloat16

C0 = 0.7978845608028654
C1 = 0.044715


def nt(a, b):
    return lax.dot_general(a, b, (((1,), (1,)), ((), ())), preferred_element_type=F32)


def cost(flops, nbytes):
    return pl.CostEstimate(flops=int(flops), bytes_accessed=int(nbytes), transcendentals=0)


def gelu_and_slope(x):
    xx = x * x
    t = jnp.tanh(x * (C0 + (C0 * C1) * xx))
    cdf = 0.5 + 0.5 * t
    return x * cdf, cdf + (0.5 * ((1.0 - t * t) * x)) * (C0 + (3.0 * C0 * C1) * xx)


def front_kernel(n, x, dy, pre, w_in, w_down, hid, d_pre, dy_all, x_la, x_rb, x_a1, x_a2, x_b1, x_b2, x_lb1, x_ra1, own, p_la, p_rb, p_lb, p_ra, p_oa, p_ob, *scratch):
    dy_buf, w_all, w_buf, pre_buf, x_buf, d_buf, hid_buf, turn_buf, out_wide, out_slim = scratch[:10]
    send_sem, recv_sem, own_sem, all_sem, w_sem, pre_sem, d_sem, hid_sem, out_sem, dy_sem, x_sem, turn_sem = scratch[10:]
    me = lax.axis_index("tp")
    right, left, far = lax.rem(me + 1, n), lax.rem(me + n - 1, n), lax.rem(me + 2, n)
    pieces, piece, _ = w_all.shape
    slots = w_buf.shape[0]
    block = 2 * piece
    steps = pieces // 2
    rows = dy.shape[0]
    half = rows // 2
    total = 4 * pieces

    barrier = pltpu.get_barrier_semaphore()
    for neighbour in (left, right):
        pl.semaphore_signal(barrier, inc=1, device_id={"tp": neighbour}, device_id_type=pl.DeviceIdType.MESH)

    def send(k, src, dst, to):
        return pltpu.make_async_remote_copy(
            src_ref=src,
            dst_ref=dst,
            send_sem=send_sem.at[k],
            recv_sem=recv_sem.at[k],
            device_id={"tp": to},
            device_id_type=pl.DeviceIdType.MESH,
        )

    up, down = pl.ds(0, half), pl.ds(half, half)
    first_part, second_part = pl.ds(0, x_a1.shape[0]), pl.ds(x_a1.shape[0], x_a2.shape[0])
    sends = [
        send(0, dy.at[up], dy_buf.at[1, up], right),
        send(1, dy.at[down], dy_buf.at[1, down], left),
        send(2, dy.at[down], dy_buf.at[2, up], right),
        send(3, dy.at[up], dy_buf.at[2, down], left),
        send(4, dy_buf.at[1, up], dy_buf.at[3, up], right),
        send(5, dy_buf.at[1, down], dy_buf.at[3, down], left),
        send(6, x_a1, x_la.at[first_part], right),
        send(7, x_b1, x_rb.at[first_part], left),
        send(8, x_a2, x_la.at[second_part], right),
        send(9, x_b2, x_rb.at[second_part], left),
        send(10, x_b1, x_lb1, right),
        send(11, x_a1, x_ra1, left),
    ]

    def columns(j):
        return pl.ds(pl.multiple_of(j * block, block), block)

    def whole_copy(j):
        return pltpu.make_async_copy(w_down.at[pl.ds(pl.multiple_of(j * piece, piece), piece)], w_all.at[j], all_sem.at[j])

    def w_start(b):
        at = lax.rem(b, pieces) * piece
        slot = lax.rem(b, slots)
        few = piece // 4
        for c in range(4):
            src = w_in.at[pl.ds(pl.multiple_of(at + c * few, few), few)]
            pltpu.make_async_copy(src, w_buf.at[slot, pl.ds(c * few, few)], w_sem.at[slot]).start()

    def w_wait(b):
        slot = lax.rem(b, slots)
        pltpu.make_async_copy(w_in.at[pl.ds(0, piece)], w_buf.at[slot], w_sem.at[slot]).wait()

    first_rows = [
        (2 * me, 2 * me + 1),
        (2 * left, 2 * right + 1),
        (2 * left + 1, 2 * right),
        (2 * far, 2 * far + 1),
    ]

    def pre_copies(s, j):
        slot = lax.rem(j, 2)
        return [
            pltpu.make_async_copy(
                pre.at[pl.ds(pl.multiple_of(first_rows[s][k] * half, half), half), columns(j)],
                pre_buf.at[slot, pl.ds(k * half, half)],
                pre_sem.at[slot, k],
            )
            for k in range(2)
        ]

    def hid_copy(s, j):
        slot = lax.rem(j, 2)
        return pltpu.make_async_copy(hid_buf.at[slot], hid.at[columns(j), pl.ds(s * rows, rows)], hid_sem.at[slot])

    def narrow(j):
        return pl.ds(pl.multiple_of(j * piece, piece), piece)

    def x_copy(j):
        slot = lax.rem(j, 2)
        return pltpu.make_async_copy(x.at[:, narrow(j)], x_buf.at[slot], x_sem.at[slot])

    early = x_a1.shape[0] // piece

    def turn_start(j):
        slot = lax.rem(j, 2)

        def to(a, b, at):
            at = pl.ds(pl.multiple_of(at * piece, piece), piece)
            pltpu.make_async_copy(turn_buf.at[slot, :, up], a.at[at], turn_sem.at[slot, 0]).start()
            pltpu.make_async_copy(turn_buf.at[slot, :, down], b.at[at], turn_sem.at[slot, 1]).start()

        @pl.when(j < early)
        def _():
            to(x_a1, x_b1, j)

        @pl.when(j >= early)
        def _():
            to(x_a2, x_b2, j - early)

    def turn_wait(j):
        slot = lax.rem(j, 2)
        at = pl.ds(0, piece)
        pltpu.make_async_copy(turn_buf.at[slot, :, up], x_a1.at[at], turn_sem.at[slot, 0]).wait()
        pltpu.make_async_copy(turn_buf.at[slot, :, down], x_b1.at[at], turn_sem.at[slot, 1]).wait()

    outs_of = [(own,), (p_la, p_rb), (p_lb, p_ra), (p_oa, p_ob)]

    def out_copies(s, j):
        slot = lax.rem(j, 2)
        buf = out_wide if s % 2 == 0 else out_slim
        at, copies = 0, []
        for k, o in enumerate(outs_of[s]):
            copies.append(pltpu.make_async_copy(buf.at[slot, pl.ds(at, o.shape[0])], o.at[:, narrow(j)], out_sem.at[s % 2, slot, k]))
            at += o.shape[0]
        return copies

    own_copy = pltpu.make_async_copy(dy, dy_buf.at[0], own_sem)
    own_copy.start()
    for copy in pre_copies(0, 0):
        copy.start()
    for j in range(2):
        whole_copy(j).start()
    pl.semaphore_wait(barrier, 2)
    for k in range(4):
        sends[k].start()
    own_copy.wait()
    for j in range(2, 4):
        whole_copy(j).start()
    for j in range(2):
        x_copy(j).start()

    for s in range(4):
        if s > 0:
            for k in (2 * s - 2, 2 * s - 1):
                sends[k].wait_recv()
            if s == 1:
                for k in range(4, 6):
                    sends[k].start()
                for j in (pieces - 2, pieces - 1):
                    turn_wait(j)
                for k in range(6, 12):
                    sends[k].start()
            keep = pltpu.make_async_copy(dy_buf.at[s], dy_all.at[pl.ds((s - 1) * rows, rows)], dy_sem.at[s - 1])
            keep.start()

        def first(j, _, s=s):
            slot = lax.rem(j, 2)

            @pl.when(j + 1 < steps)
            def _():
                for copy in pre_copies(s, j + 1):
                    copy.start()

            if s == 0:
                for c in range(2):
                    whole_copy(2 * j + c).wait()

                for c in range(2):

                    @pl.when(2 * j + c + 4 < pieces)
                    def _(c=c):
                        whole_copy(2 * j + c + 4).start()

                    @pl.when(2 * j + c + slots >= pieces)
                    def _(c=c):
                        w_start(2 * j + c + slots - pieces)

            for copy in pre_copies(s, j):
                copy.wait()

            if s == 0:

                @pl.when(j >= 2)
                def _():
                    hid_copy(s, j).wait()
            else:
                hid_copy(s, j).wait()

            for c in range(2):
                d_hid = nt(dy_buf[s], w_all[2 * j + c])
                h, slope = gelu_and_slope(pre_buf[slot, :, c * piece : (c + 1) * piece].astype(F32))
                hid_buf[slot, c * piece : (c + 1) * piece, :] = h.T.astype(BF16)
                d_buf[:, pl.ds(pl.multiple_of(j * block + c * piece, piece), piece)] = (d_hid * slope).astype(BF16)
            hid_copy(s, j).start()
            return 0

        lax.fori_loop(0, steps, first, 0)
        d_copy = pltpu.make_async_copy(d_buf, d_pre.at[pl.ds(s * rows, rows)], d_sem)
        d_copy.start()
        if s > 0:
            for j in (pieces - 2, pieces - 1):
                for copy in out_copies(s - 1, j):
                    copy.wait()
        if s < 3:
            for copy in pre_copies(s + 1, 0):
                copy.start()

        def second(j, _, s=s):
            b = s * pieces + j
            slot = lax.rem(j, 2)
            if s == 0:
                x_copy(j).wait()
            w_wait(b)

            @pl.when(j >= 2)
            def _():
                for copy in out_copies(s, j - 2):
                    copy.wait()
                if s == 0:
                    turn_wait(j)

            buf = out_wide if s % 2 == 0 else out_slim
            buf[slot] = nt(d_buf[...], w_buf[lax.rem(b, slots)]).astype(buf.dtype)
            if s == 0:
                turn_buf[slot] = x_buf[slot].T
                turn_start(j)

                @pl.when(j + 2 < pieces)
                def _():
                    x_copy(j + 2).start()

            for copy in out_copies(s, j):
                copy.start()

            @pl.when(b + slots < total)
            def _():
                w_start(b + slots)

            return 0

        lax.fori_loop(0, pieces, second, 0)
        d_copy.wait()
        if s > 0:
            keep.wait()

    for j in (pieces - 2, pieces - 1):
        for copy in out_copies(3, j):
            copy.wait()
    for j in (steps - 2, steps - 1):
        hid_copy(3, j).wait()
    for k in range(6, 12):
        sends[k].wait_recv()
    for k in range(12):
        sends[k].wait_send()


def front(n, x, dy, pre, w_in, w_down):
    rows, d = dy.shape
    tokens, ff = pre.shape
    half, piece, slots = rows // 2, 512, 3
    pieces, block = ff // piece, 2 * piece
    anywhere = pl.BlockSpec(memory_space=pl.ANY)
    dma = pltpu.SemaphoreType.DMA
    shapes = [((ff, tokens), BF16), ((tokens, ff), BF16), ((tokens - rows, d), BF16)]
    shapes += [((d, half), BF16)] * 2 + [((d // 4, half), BF16), ((d - d // 4, half), BF16)] * 2
    shapes += [((d // 4, half), BF16)] * 2 + [((rows, d), F32)]
    shapes += [((half, d), BF16)] * 2 + [((half, d), F32)] * 2 + [((half, d), BF16)] * 2
    out_shape = [jax.ShapeDtypeStruct(*t) for t in shapes]
    return pl.pallas_call(
        functools.partial(front_kernel, n),
        in_specs=[anywhere] * 5,
        out_specs=[anywhere] * len(out_shape),
        scratch_shapes=[
            pltpu.VMEM((4, rows, d), BF16),
            pltpu.VMEM((pieces, piece, d), BF16),
            pltpu.VMEM((slots, piece, ff), BF16),
            pltpu.VMEM((2, rows, block), BF16),
            pltpu.VMEM((2, rows, piece), BF16),
            pltpu.VMEM((rows, ff), BF16),
            pltpu.VMEM((2, block, rows), BF16),
            pltpu.VMEM((2, piece, rows), BF16),
            pltpu.VMEM((2, rows, piece), F32),
            pltpu.VMEM((2, rows, piece), BF16),
            dma((12,)),
            dma((12,)),
            dma,
            dma((pieces,)),
            dma((slots,)),
            dma((2, 2)),
            dma,
            dma((2,)),
            dma((2, 2, 2)),
            dma((3,)),
            dma((2,)),
            dma((2, 2)),
        ],
        out_shape=out_shape,
        compiler_params=pltpu.CompilerParams(collective_id=0, has_side_effects=True, vmem_limit_bytes=67043328),
        cost_estimate=cost(4 * tokens * ff * d, 10 * ff * d),
        name="front",
    )(x, dy, pre, w_in, w_down)


def dw_kernel(n_lhs, n_rhs, *refs):
    lhs = [r[...] for r in refs[:n_lhs]]
    rhs = [r[...] for r in refs[n_lhs : n_lhs + n_rhs]]
    lhs = lhs[0] if n_lhs == 1 else jnp.concatenate(lhs, axis=1)
    rhs = rhs[0] if n_rhs == 1 else jnp.concatenate(rhs, axis=0)
    refs[-1][...] = jnp.dot(lhs, rhs, preferred_element_type=F32).astype(BF16)


def dw_of(lhs, rhs, room, rows=None, into=None):
    m, n = max(t.shape[0] for t in lhs), rhs[0].shape[1]
    low, high = rows or (0, m)
    k = sum(t.shape[0] for t in rhs)
    bm, bn = min(1024, high - low), min(2048, n)
    first = low // bm
    more = [] if into is None else [into]

    def at(t):
        return first if t.shape[0] == m else 0

    return pl.pallas_call(
        functools.partial(dw_kernel, len(lhs), len(rhs)),
        grid=((high - low) // bm, n // bn),
        in_specs=[pl.BlockSpec((bm, t.shape[1]), lambda i, j, s=at(t): (s + i, 0)) for t in lhs]
        + [pl.BlockSpec((t.shape[0], bn), lambda i, j: (0, j)) for t in rhs]
        + [pl.BlockSpec(memory_space=pl.ANY) for _ in more],
        out_specs=pl.BlockSpec((bm, bn), lambda i, j: (first + i, j)),
        out_shape=jax.ShapeDtypeStruct((m, n), BF16),
        input_output_aliases={len(lhs) + len(rhs): 0} if more else {},
        compiler_params=pltpu.CompilerParams(vmem_limit_bytes=room << 20),
        cost_estimate=cost(2 * (high - low) * n * k, 2 * (high - low) * n),
    )(*lhs, *rhs, *more)


def last_kernel(sum_ref, over_left, over_right, o_ref):
    half = over_left.shape[0]
    o_ref[:half, :] = (sum_ref[:half, :] + over_left[...].astype(F32)).astype(BF16)
    o_ref[half:, :] = (sum_ref[half:, :] + over_right[...].astype(F32)).astype(BF16)


def near_kernel(own_ref, from_right, from_left, o_ref):
    half = from_left.shape[0]
    o_ref[:half, :] = own_ref[:half, :] + from_right[...].astype(F32)
    o_ref[half:, :] = own_ref[half:, :] + from_left[...].astype(F32)


def sum_of(kernel, whole, top, low, dtype):
    rows, d = whole.shape
    half, bd = rows // 2, min(1024, d)
    piece = pl.BlockSpec((half, bd), lambda j: (0, j))
    full = pl.BlockSpec((rows, bd), lambda j: (0, j))
    return pl.pallas_call(
        kernel,
        grid=(d // bd,),
        in_specs=[full, piece, piece],
        out_specs=full,
        out_shape=jax.ShapeDtypeStruct((rows, d), dtype),
        compiler_params=pltpu.CompilerParams(vmem_limit_bytes=16 << 20),
        cost_estimate=cost(rows * d * 100, rows * d * 10),
    )(whole, top, low)


def solution(mesh):
    n = mesh.shape["tp"]
    to_right = [(i, (i + 1) % n) for i in range(n)]
    to_left = [(i, (i - 1) % n) for i in range(n)]

    def right(t):
        return lax.ppermute(t, "tp", to_right)

    def left(t):
        return lax.ppermute(t, "tp", to_left)

    def step(x, dy, pre, w_in, w_down):
        (hid, d_pre, dy_all, x_la, x_rb, x_a1, x_a2, x_b1, x_b2, x_lb1, x_ra1, own, *parts) = front(
            n, x, dy, pre, w_in, w_down
        )
        p_la, p_rb, p_lb, p_ra, p_oa, p_ob = parts
        x_lb2 = right(x_b2)
        x_ra2 = left(x_a2)
        x_oa = right(x_la)
        x_ob = left(x_rb)

        in_l = right(p_oa)
        in_r = left(p_ob)
        from_left = right(p_rb)
        from_right = left(p_la)
        over_left = right((p_ra + in_l.astype(F32)).astype(BF16))
        over_right = left((p_lb + in_r.astype(F32)).astype(BF16))

        dw_down = dw_of([hid], [dy, dy_all], 52)
        d, cut = x_la.shape[0], x_a1.shape[0]
        xs = [x_a1, x_b1, x_la, x_rb, x_lb1, x_ra1, x_oa, x_ob]
        dw_in = dw_of(xs, [d_pre], 28, (0, cut))
        xs = [x_a2, x_b2, x_la, x_rb, x_lb2, x_ra2, x_oa, x_ob]
        dw_in = dw_of(xs, [d_pre], 28, (cut, d), dw_in)
        near = sum_of(near_kernel, own, from_right, from_left, F32)
        dx = sum_of(last_kernel, near, over_left, over_right, BF16)
        return dx, dw_in, dw_down

    return jax.shard_map(
        step,
        mesh=mesh,
        in_specs=(P(("dp", "tp"), None), P(("dp", "tp"), None), P("dp", "tp"), P(None, "tp"), P("tp", None)),
        out_specs=(P(("dp", "tp"), None), P("dp", "tp"), P(("dp", "tp"), None)),
        check_vma=False,
    )
```
